32 devices in a mesh: frames: 8 (over z, x), heads: 4 (over y, core).
Axes of the slice: x: 2, y: 2, z: 4, core: 2. Of those that a mesh axis runs over, the one named last changes fastest.
Arguments:
- queries: bfloat16 [8192, 2560], P('frames', 'heads'), may hold values from -6 to 6, as said below
- keys: bfloat16 [8192, 2560], P('frames', 'heads'), may hold values from -6 to 6, as said below
- values: bfloat16 [8192, 2560], P('frames', 'heads'), may hold values from -6 to 6
- block_ids: int32 [64, 4], replicated, may hold values from 0 to 63, as said below
- counts: int32 [64], P('frames'), may hold values from 1 to 4
- w_out: bfloat16 [2560, 5120], P('heads'), may hold values from -0.125 to 0.125
Outputs:
- projected: bfloat16 [8192, 5120], P('frames', 'heads')
The draws below stay inside these ranges and needn't reach their ends.
Inputs may be any that keep to these rules, and one draw needn't show every extreme that they name: `block_ids`: block j is held by index j // 8 of frames. Counted with repeats, the entries of the 8 query blocks of one index of frames name at most 4 blocks held by any one index, and exactly 4 held by some index. Entries of a row may repeat. `queries`: drawn in float32 and rounded once. `keys`: drawn in float32 and rounded once.
All inputs are finite; a program needn't handle non-finite values.
Results may differ from the reference program's by a relative error of at most 0.0052.
Values may be sent and summed in bfloat16 or wider, within the bound.
A program may use at most 192 MiB of HBM per device.

```python
import jax
import jax.numpy as jnp
from jax import lax

D = 5120
HEADS = 20
DH = 128
TILE = 128
SEL = 4
BLK_DEV = 8
NB = 64
TOKENS = 8192
CAP = 4
N_FRAMES = 8


def pair_draw(key, which_one):
    base = jax.random.fold_in(key, 7)
    key_query, key_key = jax.random.split(base, 2)
    full_shape = (TOKENS, HEADS * DH)
    query_part = jnp.clip(1.5 * jax.random.normal(key_query, full_shape, jnp.float32), -6.0, 6.0)
    key_part = jnp.clip(1.5 * jax.random.normal(key_key, full_shape, jnp.float32), -6.0, 6.0)
    if which_one == 0:
        return query_part
    return key_part


def draw_queries(key, part):
    return pair_draw(key, 0).astype(jnp.bfloat16)


def draw_keys(key, part):
    return pair_draw(key, 1).astype(jnp.bfloat16)


def draw_block_ids(key, part):
    requests = BLK_DEV * SEL

    def one_device(device_key):
        key_star, key_order, key_shuffle, key_local = jax.random.split(device_key, 4)
        owners = jnp.tile(jnp.arange(N_FRAMES, dtype=jnp.int32), CAP)
        star = jax.random.randint(key_star, (), 0, N_FRAMES, dtype=jnp.int32)
        order = jax.random.permutation(key_order, N_FRAMES * CAP).astype(jnp.int32)
        priority = order + jnp.where(owners == star, 0, N_FRAMES * CAP).astype(jnp.int32)
        picked = owners[jnp.argsort(priority, stable=True)][:requests]
        shuffled = picked[jax.random.permutation(key_shuffle, requests)]
        local_block = jax.random.randint(key_local, (requests,), 0, BLK_DEV, dtype=jnp.int32)
        return shuffled * BLK_DEV + local_block
    device_keys = jax.vmap(lambda device: jax.random.fold_in(key, 100 + device))(jnp.arange(N_FRAMES))
    return jax.vmap(one_device)(device_keys).reshape(NB, SEL).astype(jnp.int32)


def place_ends(array, key, least, top_value):
    spot = [jax.random.randint(jax.random.fold_in(key, axis), (), 0, length) for axis, length in enumerate(array.shape)]
    main_axis = array.shape.index(max(array.shape))
    beside = spot[:main_axis] + [(spot[main_axis] + 1) % array.shape[main_axis]] + spot[main_axis + 1:]
    return array.at[tuple(spot)].set(least).at[tuple(beside)].set(top_value)


def level_of(own_key, shape, cuts, least, top_value):
    def one(axis_at, shards_of):
        draws = jax.random.uniform(jax.random.fold_in(jax.random.fold_in(own_key, 6), axis_at), (shards_of,), jnp.float32, least / len(cuts), top_value / len(cuts))
        return jnp.repeat(jnp.exp(draws), shape[axis_at] // shards_of).reshape((-1,) + (1,) * (len(shape) - axis_at - 1))

    loudness = one(*cuts[0])
    for cut in cuts[1:]:
        loudness = loudness * one(*cut)
    return loudness


def normal_values(key, extent, scale, reach, cuts=(), kind=jnp.bfloat16):
    loudness = level_of(key, extent, cuts, -0.22, 0.18) if cuts else 1.0
    array = jax.random.normal(key, extent, jnp.float32) * scale * loudness
    return jnp.minimum(jnp.maximum(array, -reach), reach).astype(kind)


def setup_inputs(seed: int = 0) -> dict:
    arg_keys = jax.random.split(jax.random.key(seed), 7)
    queries = draw_queries(jax.random.fold_in(arg_keys[6], 71), 0)
    keys = draw_keys(jax.random.fold_in(arg_keys[6], 71), 0)
    values = normal_values(arg_keys[2], (TOKENS, HEADS * DH), 1.0, 6.0, ((0, 8), (1, 4)))
    block_ids = draw_block_ids(jax.random.fold_in(arg_keys[6], 71), 0)
    counts = place_ends(jax.random.randint(arg_keys[4], (NB,), 1, SEL + 1), jax.random.fold_in(arg_keys[4], 1), 1, SEL).astype(jnp.int32)
    w_out = normal_values(arg_keys[5], (HEADS * DH, D), (HEADS * DH) ** -0.5, 0.125, ((0, 4),))
    return {"queries": queries, "keys": keys, "values": values, "block_ids": block_ids, "counts": counts, "w_out": w_out}


def reference(queries, keys, values, block_ids, counts, w_out):
    full_width = HEADS * DH
    inv_root = 1.0 / (DH ** 0.5)
    query_tiles = queries.reshape(NB, TILE, full_width)
    key_tiles = keys.reshape(NB, TILE, full_width)
    value_tiles = values.reshape(NB, TILE, full_width)

    def one_block(block_index):
        chosen = block_ids[block_index]
        keyset_k = jnp.concatenate([key_tiles[block_index][None], key_tiles[chosen]], 0)
        keyset_v = jnp.concatenate([value_tiles[block_index][None], value_tiles[chosen]], 0)
        keyset_k = keyset_k.reshape((SEL + 1) * TILE, HEADS, DH).astype(jnp.float32)
        keyset_v = keyset_v.reshape((SEL + 1) * TILE, HEADS, DH).astype(jnp.float32)
        query_tile = query_tiles[block_index].reshape(TILE, HEADS, DH).astype(jnp.float32)
        scores = jnp.einsum("qhd,khd->hqk", query_tile, keyset_k) * inv_root
        allowed = jnp.concatenate([jnp.ones((1,), bool), jnp.arange(SEL) < counts[block_index]])
        key_allowed = jnp.repeat(allowed, TILE)
        scores = jnp.where(key_allowed[None, None, :], scores, -jnp.inf)
        row_max = jnp.max(scores, axis=-1, keepdims=True)
        probs = jnp.exp(scores - row_max)
        denom_sum = jnp.sum(probs, axis=-1)
        weights = lax.optimization_barrier(probs.astype(jnp.bfloat16)).astype(jnp.float32)
        mixed = jnp.einsum("hqk,khd->qhd", weights, keyset_v)
        mixed = mixed / jnp.transpose(denom_sum)[:, :, None]
        return mixed.astype(jnp.bfloat16).reshape(TILE, full_width)

    attn = lax.map(one_block, jnp.arange(NB)).reshape(TOKENS, full_width)
    return jnp.dot(attn, w_out, preferred_element_type=jnp.float32).astype(jnp.bfloat16)
```

```python
import functools

import jax
import jax.numpy as jnp
from jax import lax
from jax.experimental import pallas as pl
from jax.experimental.pallas import tpu as pltpu
from jax.sharding import PartitionSpec as P

DH = 128
TILE = 128
MESH = pl.DeviceIdType.MESH
F32 = jnp.float32
NT_DIMS = (((1,), (1,)), ((), ()))


def layer_kernel(
    dims, pick_ref, slot_ref, count_ref, q_ref, k_ref, v_ref, w_ref, out_ref,
    send, rows, attn, acc, kv_send, kv_recv, w_send, w_recv, a_send, a_recv, own_sem, *recv,
):
    frames, peers, blocks, select, capacity, heads, slots = dims
    me_f, me_p = lax.axis_index("frames"), lax.axis_index("heads")
    depth = heads * DH
    features = rows.shape[2]

    barrier = pltpu.get_barrier_semaphore()

    @pl.loop(1, frames)
    def _(step):
        pl.semaphore_signal(
            barrier, inc=1, device_id=(lax.rem(me_f + step, frames), me_p), device_id_type=MESH
        )

    @pl.loop(1, peers)
    def _(step):
        pl.semaphore_signal(
            barrier, inc=1, device_id=(me_f, lax.rem(me_p + step, peers)), device_id_type=MESH
        )

    def columns_of(peer):
        return pl.ds(pl.multiple_of(peer * features, features), features)

    own_rows = pltpu.make_async_copy(w_ref.at[:, columns_of(me_p)], rows.at[me_p], own_sem)
    own_rows.start()

    def head_columns(h):
        return slice(h * DH, (h + 1) * DH)

    def kv_copy(h, target, origin):
        return pltpu.make_async_remote_copy(
            src_ref=send.at[h % slots, target],
            dst_ref=recv[h].at[pl.ds(origin * capacity, capacity)],
            send_sem=kv_send.at[h, target],
            recv_sem=kv_recv.at[h, origin],
            device_id=(target, me_p),
            device_id_type=MESH,
        )

    def build_kv(h):
        if h >= slots:

            @pl.loop(1, frames)
            def _(step):
                kv_copy(h - slots, lax.rem(me_f + step, frames), me_f).wait_send()

        @pl.loop(1, frames)
        def _(step):
            target = lax.rem(me_f + step, frames)
            for c in range(capacity):
                index = pick_ref[target * capacity + c]
                send[h % slots, target, c, 0] = k_ref[index, :, head_columns(h)]
                send[h % slots, target, c, 1] = v_ref[index, :, head_columns(h)]

        for c in range(capacity):
            index = pick_ref[me_f * capacity + c]
            recv[h][me_f * capacity + c, 0] = k_ref[index, :, head_columns(h)]
            recv[h][me_f * capacity + c, 1] = v_ref[index, :, head_columns(h)]

    def start_kv(h):
        @pl.loop(1, frames)
        def _(step):
            kv_copy(h, lax.rem(me_f + step, frames), me_f).start()

    def wait_kv(h):
        @pl.loop(1, frames)
        def _(step):
            origin = lax.rem(me_f + step, frames)
            kv_copy(h, origin, origin).wait_recv()

    def w_copy(target, origin):
        return pltpu.make_async_remote_copy(
            src_ref=w_ref.at[:, columns_of(target)],
            dst_ref=rows.at[origin],
            send_sem=w_send.at[target],
            recv_sem=w_recv.at[origin],
            device_id=(me_f, target),
            device_id_type=MESH,
        )

    def a_copy(h, target, origin):
        return pltpu.make_async_remote_copy(
            src_ref=attn.at[h, me_p],
            dst_ref=attn.at[h, origin],
            send_sem=a_send.at[h, target],
            recv_sem=a_recv.at[h, origin],
            device_id=(me_f, target),
            device_id_type=MESH,
        )

    def over_peers(action):
        @pl.loop(1, peers)
        def _(step):
            action(lax.rem(me_p + step, peers))

    def attend(h):
        @pl.loop(0, blocks)
        def _(b):
            q = q_ref[b, :, head_columns(h)]
            picks = [slot_ref[b * select + s] for s in range(select)]
            keyset = jnp.concatenate(
                [k_ref[b, :, head_columns(h)]] + [recv[h][i, 0] for i in picks], axis=0
            )
            valueset = jnp.concatenate(
                [v_ref[b, :, head_columns(h)]] + [recv[h][i, 1] for i in picks], axis=0
            )
            scores = lax.dot_general(q, keyset, NT_DIMS, preferred_element_type=F32)
            scores = scores * (1.0 / DH**0.5)
            position = lax.broadcasted_iota(jnp.int32, scores.shape, 1)
            scores = jnp.where(position < (count_ref[b] + 1) * TILE, scores, -jnp.inf)
            top = jnp.max(scores, axis=1, keepdims=True)
            probs = jnp.exp(scores - top)
            denom = jnp.sum(probs, axis=1, keepdims=True)
            mixed = jnp.dot(probs.astype(jnp.bfloat16), valueset, preferred_element_type=F32)
            attn[h, me_p, pl.ds(pl.multiple_of(b * TILE, TILE), TILE), :] = (mixed / denom).astype(
                jnp.bfloat16
            )

    row_tile = 2 * TILE

    def project(h):
        @pl.loop(0, blocks * TILE // row_tile)
        def _(r):
            span = pl.ds(pl.multiple_of(r * row_tile, row_tile), row_tile)
            left = jnp.concatenate([attn[h, p, span, :] for p in range(peers)], axis=1)
            right = jnp.concatenate([rows[p, head_columns(h), :] for p in range(peers)], axis=0)
            term = jnp.dot(left, right, preferred_element_type=F32)
            if h > 0:
                term = term + acc[span, :]
            if h == heads - 1:
                out_ref[span, :] = term.astype(out_ref.dtype)
            else:
                acc[span, :] = term

    build_kv(0)
    pl.semaphore_wait(barrier, frames + peers - 2)
    start_kv(0)
    over_peers(lambda target: w_copy(target, me_p).start())
    if heads > 1:
        build_kv(1)
        start_kv(1)
    for h in range(heads):
        if h + 2 < heads:
            build_kv(h + 2)
        wait_kv(h)
        if h + 2 < heads:
            start_kv(h + 2)
        attend(h)
        over_peers(lambda target: a_copy(h, target, me_p).start())
        if h == 0:
            own_rows.wait()
            over_peers(lambda origin: w_copy(origin, origin).wait_recv())
        else:
            over_peers(lambda origin: a_copy(h - 1, origin, origin).wait_recv())
            project(h - 1)
    over_peers(lambda origin: a_copy(heads - 1, origin, origin).wait_recv())
    project(heads - 1)
    for h in range(max(0, heads - slots), heads):

        @pl.loop(1, frames)
        def _(step):
            kv_copy(h, lax.rem(me_f + step, frames), me_f).wait_send()

    over_peers(lambda target: w_copy(target, me_p).wait_send())
    for h in range(heads):
        over_peers(lambda target: a_copy(h, target, me_p).wait_send())


def shards(queries, keys, values, block_ids, counts, w_out):
    frames = lax.axis_size("frames")
    peers = lax.axis_size("heads")
    here = lax.axis_index("frames")
    tokens, width = queries.shape
    blocks = tokens // TILE
    select = block_ids.shape[1]
    heads = width // DH
    requests = blocks * select
    capacity = max(2, (requests + frames - 1) // frames)
    features = w_out.shape[1] // peers
    slots = min(3, heads)

    ids = block_ids.reshape(frames, requests)
    owner = ids // blocks
    local = ids % blocks
    mine = owner == here
    order = jnp.arange(requests, dtype=jnp.int32)
    before = order[:, None] < order[None, :]
    rank = jnp.sum((mine[:, :, None] & before[None]).astype(jnp.int32), axis=1)
    hit = mine[:, :, None] & (rank[:, :, None] == jnp.arange(capacity, dtype=jnp.int32))
    pick = jnp.sum(jnp.where(hit, local[:, :, None], 0), axis=1).reshape(-1)
    my_owner = lax.dynamic_slice_in_dim(owner, here, 1, 0).reshape(requests)
    same = (my_owner[:, None] == my_owner[None, :]) & before
    my_slot = my_owner * capacity + jnp.sum(same.astype(jnp.int32), axis=0)

    smem = pl.BlockSpec(memory_space=pltpu.SMEM)
    vmem = pl.BlockSpec(memory_space=pltpu.VMEM)
    tiles = (blocks, TILE, width)
    dma = pltpu.SemaphoreType.DMA
    return pl.pallas_call(
        functools.partial(layer_kernel, (frames, peers, blocks, select, capacity, heads, slots)),
        out_shape=jax.ShapeDtypeStruct((tokens, features), jnp.bfloat16),
        in_specs=[smem, smem, smem, vmem, vmem, vmem, pl.BlockSpec(memory_space=pl.ANY)],
        out_specs=vmem,
        scratch_shapes=[
            pltpu.VMEM((slots, frames, capacity, 2, TILE, DH), jnp.bfloat16),
            pltpu.VMEM((peers, width, features), jnp.bfloat16),
            pltpu.VMEM((heads, peers, tokens, DH), jnp.bfloat16),
            pltpu.VMEM((tokens, features), F32),
            dma((heads, frames)),
            dma((heads, frames)),
            dma((peers,)),
            dma((peers,)),
            dma((heads, peers)),
            dma((heads, peers)),
            dma,
        ]
        + [pltpu.VMEM((frames * capacity, 2, TILE, DH), jnp.bfloat16)] * heads,
        compiler_params=pltpu.CompilerParams(
            collective_id=0, has_side_effects=True, vmem_limit_bytes=67043328
        ),
    )(
        pick, my_slot, counts, queries.reshape(tiles), keys.reshape(tiles), values.reshape(tiles),
        w_out,
    )


def solution(mesh):
    placed = (
        P("frames", "heads"),
        P("frames", "heads"),
        P("frames", "heads"),
        P(),
        P("frames"),
        P("heads", None),
    )
    return jax.shard_map(
        shards, mesh=mesh, in_specs=placed, out_specs=P("frames", "heads"), check_vma=False
    )
```

```python
import functools
import math

import jax
import jax.numpy as jnp
from jax import lax
from jax.experimental import pallas as pl
from jax.experimental.pallas import tpu as pltpu
from jax.sharding import PartitionSpec as P

DH = 128
TILE = 128
MESH = pl.DeviceIdType.MESH
F32 = jnp.float32
PAIR = 2
AHEAD = 2
VMEM_BYTES = 67043328
NT_DIMS = (((1,), (1,)), ((), ()))


def head_columns(h):
    return slice(h * DH, (h + 1) * DH)


class direct_exchange:
    def __init__(self, dims, pick_ref, k_ref, v_ref, recv, send, kv_send, kv_recv):
        self.frames, _, _, _, self.capacity, self.heads, self.slots = dims
        self.pick_ref, self.k_ref, self.v_ref, self.recv = pick_ref, k_ref, v_ref, recv
        self.send, self.kv_send, self.kv_recv = send, kv_send, kv_recv
        self.me_f, self.me_p = lax.axis_index("frames"), lax.axis_index("heads")

    def copy(self, h, target, origin):
        return pltpu.make_async_remote_copy(
            src_ref=self.send.at[h % self.slots, target],
            dst_ref=self.recv[h].at[pl.ds(origin * self.capacity, self.capacity)],
            send_sem=self.kv_send.at[h, target],
            recv_sem=self.kv_recv.at[h, origin],
            device_id=(target, self.me_p),
            device_id_type=MESH,
        )

    def others(self, action):
        @pl.loop(1, self.frames)
        def _(step):
            action(lax.rem(self.me_f + step, self.frames))

    def pick(self, target, c):
        return self.pick_ref[(target * self.frames + self.me_f) * self.capacity + c]

    def build(self, h):
        if h >= self.slots:
            self.others(lambda target: self.copy(h - self.slots, target, self.me_f).wait_send())

        def fill(target):
            for c in range(self.capacity):
                index = self.pick(target, c)
                self.send[h % self.slots, target, c, 0] = self.k_ref[index, :, head_columns(h)]
                self.send[h % self.slots, target, c, 1] = self.v_ref[index, :, head_columns(h)]

        self.others(fill)
        for c in range(self.capacity):
            index = self.pick(self.me_f, c)
            self.recv[h][self.me_f * self.capacity + c, 0] = self.k_ref[index, :, head_columns(h)]
            self.recv[h][self.me_f * self.capacity + c, 1] = self.v_ref[index, :, head_columns(h)]

    def start(self, h):
        self.others(lambda target: self.copy(h, target, self.me_f).start())

    def prepare(self):
        self.build(0)

    def begin(self):
        self.start(0)

    def follow(self):
        if self.heads > 1:
            self.build(1)
            self.start(1)

    def receive(self, h):
        if h + 2 < self.heads:
            self.build(h + 2)
        self.others(lambda origin: self.copy(h, origin, origin).wait_recv())
        if h + 2 < self.heads:
            self.start(h + 2)

    def drain(self):
        for h in range(max(0, self.heads - self.slots), self.heads):
            self.others(lambda target: self.copy(h, target, self.me_f).wait_send())


class relay_exchange:
    def __init__(
        self, dims, pick_ref, k_ref, v_ref, recv,
        picked, up_send, up_recv, down_send, down_recv, x_send, x_recv, *passing,
    ):
        self.frames, _, self.blocks, _, self.capacity, self.heads, _ = dims
        self.line = self.frames // PAIR
        self.pick_ref, self.k_ref, self.v_ref, self.recv = pick_ref, k_ref, v_ref, recv
        self.picked, self.x_send, self.x_recv = picked, x_send, x_recv
        self.sems = ((up_send, up_recv), (down_send, down_recv))
        self.passing = passing
        self.me_f, self.me_p = lax.axis_index("frames"), lax.axis_index("heads")
        self.z, self.x = self.me_f // PAIR, self.me_f % PAIR
        self.partner = self.z * PAIR + (PAIR - 1 - self.x)

    def held(self, h, way, far):
        return self.passing[(h * 2 + way) * (self.line - 1) + far - 1]

    def at(self, way, steps):
        return self.z + steps if way == 0 else self.z - steps

    def inside(self, position):
        return (position >= 0) & (position < self.line)

    def onward(self, h, way, far, kv):
        source = (self.k_ref, self.v_ref)[kv].at[:, :, head_columns(h)]
        if far > 0:
            source = self.held(h, way, far).at[kv]
        send_sem, recv_sem = self.sems[way]
        return pltpu.make_async_remote_copy(
            src_ref=source,
            dst_ref=self.held(h, way, far + 1).at[kv],
            send_sem=send_sem.at[h, far, kv],
            recv_sem=recv_sem.at[h, far, kv],
            device_id=(self.at(way, 1) * PAIR + self.x, self.me_p),
            device_id_type=MESH,
        )

    def beside(self, h, origin_z, column):
        return pltpu.make_async_remote_copy(
            src_ref=self.picked.at[h, origin_z],
            dst_ref=self.recv[h].at[
                pl.ds((origin_z * PAIR + column) * self.capacity, self.capacity)
            ],
            send_sem=self.x_send.at[h, origin_z],
            recv_sem=self.x_recv.at[h, origin_z],
            device_id=(self.partner, self.me_p),
            device_id_type=MESH,
        )

    def send_on(self, h, way, far):
        @pl.when(self.inside(self.at(way, 1)))
        def _():
            for kv in range(2):
                self.onward(h, way, far, kv).start()

    def hand_out(self, h, origin_z, load):
        origin = origin_z * PAIR + self.x
        for c in range(self.capacity):
            theirs = self.pick_ref[(self.partner * self.frames + origin) * self.capacity + c]
            for kv in range(2):
                self.picked[h, origin_z, c, kv] = load(kv, theirs)
        for c in range(self.capacity):
            ours = self.pick_ref[(self.me_f * self.frames + origin) * self.capacity + c]
            for kv in range(2):
                self.recv[h][origin * self.capacity + c, kv] = load(kv, ours)
        self.beside(h, origin_z, self.x).start()

    def own(self, h):
        def load(kv, index):
            return (self.k_ref, self.v_ref)[kv][index, :, head_columns(h)]

        self.hand_out(h, self.z, load)

    def arrive(self, h, far):
        for way in range(2):
            @pl.when(self.inside(self.at(way, -far)))
            def _():
                for kv in range(2):
                    self.onward(h, way, far - 1, kv).wait_recv()
                if far + 1 < self.line:
                    self.send_on(h, way, far)

        for way in range(2):
            @pl.when(self.inside(self.at(way, -far)))
            def _():
                held = self.held(h, way, far)
                self.hand_out(h, self.at(way, -far), lambda kv, index: held[kv, index])

    def prepare(self):
        pass

    def begin(self):
        for h in range(min(AHEAD, self.heads)):
            for way in range(2):
                self.send_on(h, way, 0)

    def follow(self):
        self.own(0)

    def receive(self, h):
        for far in range(1, self.line):
            self.arrive(h, far)
            if far == 1 and h + AHEAD < self.heads:
                for way in range(2):
                    self.send_on(h + AHEAD, way, 0)
        if h + 1 < self.heads:
            self.own(h + 1)

        @pl.loop(0, self.line)
        def _(origin_z):
            self.beside(h, origin_z, PAIR - 1 - self.x).wait_recv()

    def drain(self):
        for h in range(self.heads):
            for way in range(2):
                for far in range(self.line - 1):
                    @pl.when(self.inside(self.at(way, -far)) & self.inside(self.at(way, 1)))
                    def _():
                        for kv in range(2):
                            self.onward(h, way, far, kv).wait_send()

            @pl.loop(0, self.line)
            def _(origin_z):
                self.beside(h, origin_z, self.x).wait_send()


def layer_kernel(
    dims, relayed, pick_ref, slot_ref, count_ref, q_ref, k_ref, v_ref, w_ref, out_ref,
    rows, attn, acc, w_send, w_recv, a_send, a_recv, own_sem, *kv_refs,
):
    frames, peers, blocks, select, capacity, heads, slots = dims
    recv, kv_refs = kv_refs[:heads], kv_refs[heads:]
    me_f, me_p = lax.axis_index("frames"), lax.axis_index("heads")
    depth = heads * DH
    features = rows.shape[2]

    barrier = pltpu.get_barrier_semaphore()

    @pl.loop(1, frames)
    def _(step):
        pl.semaphore_signal(
            barrier, inc=1, device_id=(lax.rem(me_f + step, frames), me_p), device_id_type=MESH
        )

    @pl.loop(1, peers)
    def _(step):
        pl.semaphore_signal(
            barrier, inc=1, device_id=(me_f, lax.rem(me_p + step, peers)), device_id_type=MESH
        )

    def columns_of(peer):
        return pl.ds(pl.multiple_of(peer * features, features), features)

    own_rows = pltpu.make_async_copy(w_ref.at[:, columns_of(me_p)], rows.at[me_p], own_sem)
    own_rows.start()

    exchange = (relay_exchange if relayed else direct_exchange)(
        dims, pick_ref, k_ref, v_ref, recv, *kv_refs
    )

    def w_copy(target, origin):
        return pltpu.make_async_remote_copy(
            src_ref=w_ref.at[:, columns_of(target)],
            dst_ref=rows.at[origin],
            send_sem=w_send.at[target],
            recv_sem=w_recv.at[origin],
            device_id=(me_f, target),
            device_id_type=MESH,
        )

    def a_copy(h, target, origin):
        return pltpu.make_async_remote_copy(
            src_ref=attn.at[h, me_p],
            dst_ref=attn.at[h, origin],
            send_sem=a_send.at[h, target],
            recv_sem=a_recv.at[h, origin],
            device_id=(me_f, target),
            device_id_type=MESH,
        )

    def over_peers(action):
        @pl.loop(1, peers)
        def _(step):
            action(lax.rem(me_p + step, peers))

    def attend(h):
        @pl.loop(0, blocks)
        def _(b):
            q = q_ref[b, :, head_columns(h)]
            picks = [slot_ref[b * select + s] for s in range(select)]
            keyset = jnp.concatenate(
                [k_ref[b, :, head_columns(h)]] + [recv[h][i, 0] for i in picks], axis=0
            )
            valueset = jnp.concatenate(
                [v_ref[b, :, head_columns(h)]] + [recv[h][i, 1] for i in picks], axis=0
            )
            scores = lax.dot_general(q, keyset, NT_DIMS, preferred_element_type=F32)
            scores = scores * (1.0 / DH**0.5)
            position = lax.broadcasted_iota(jnp.int32, scores.shape, 1)
            scores = jnp.where(position < (count_ref[b] + 1) * TILE, scores, -jnp.inf)
            top = jnp.max(scores, axis=1, keepdims=True)
            probs = jnp.exp(scores - top)
            denom = jnp.sum(probs, axis=1, keepdims=True)
            mixed = jnp.dot(probs.astype(jnp.bfloat16), valueset, preferred_element_type=F32)
            attn[h, me_p, pl.ds(pl.multiple_of(b * TILE, TILE), TILE), :] = (mixed / denom).astype(
                jnp.bfloat16
            )

    row_tile = 2 * TILE

    def project(h):
        @pl.loop(0, blocks * TILE // row_tile)
        def _(r):
            span = pl.ds(pl.multiple_of(r * row_tile, row_tile), row_tile)
            left = jnp.concatenate([attn[h, p, span, :] for p in range(peers)], axis=1)
            right = jnp.concatenate([rows[p, head_columns(h), :] for p in range(peers)], axis=0)
            term = jnp.dot(left, right, preferred_element_type=F32)
            if h > 0:
                term = term + acc[span, :]
            if h == heads - 1:
                out_ref[span, :] = term.astype(out_ref.dtype)
            else:
                acc[span, :] = term

    exchange.prepare()
    pl.semaphore_wait(barrier, frames + peers - 2)
    exchange.begin()
    over_peers(lambda target: w_copy(target, me_p).start())
    exchange.follow()
    for h in range(heads):
        exchange.receive(h)
        attend(h)
        over_peers(lambda target: a_copy(h, target, me_p).start())
        if h == 0:
            own_rows.wait()
            over_peers(lambda origin: w_copy(origin, origin).wait_recv())
        else:
            over_peers(lambda origin: a_copy(h - 1, origin, origin).wait_recv())
            project(h - 1)
    over_peers(lambda origin: a_copy(heads - 1, origin, origin).wait_recv())
    project(heads - 1)
    exchange.drain()
    over_peers(lambda target: w_copy(target, me_p).wait_send())
    for h in range(heads):
        over_peers(lambda target: a_copy(h, target, me_p).wait_send())


def shards(queries, keys, values, block_ids, counts, w_out):
    frames = lax.axis_size("frames")
    peers = lax.axis_size("heads")
    here = lax.axis_index("frames")
    tokens, width = queries.shape
    blocks = tokens // TILE
    select = block_ids.shape[1]
    heads = width // DH
    requests = blocks * select
    capacity = max(2, (requests + frames - 1) // frames)
    features = w_out.shape[1] // peers
    slots = min(3, heads)

    ids = block_ids.reshape(frames, requests)
    owner = ids // blocks
    order = jnp.arange(requests, dtype=jnp.int32)
    same = (owner[:, :, None] == owner[:, None, :]) & (order[:, None] < order[None, :])
    slot = owner * capacity + jnp.sum(same.astype(jnp.int32), axis=1)
    hit = slot[:, None, :] == jnp.arange(frames * capacity, dtype=jnp.int32)[:, None]
    pick = jnp.sum(jnp.where(hit, (ids % blocks)[:, None, :], 0), axis=2).reshape(-1)
    my_slot = lax.dynamic_slice_in_dim(slot, here, 1, 0).reshape(requests)

    smem = pl.BlockSpec(memory_space=pltpu.SMEM)
    vmem = pl.BlockSpec(memory_space=pltpu.VMEM)
    tiles = (blocks, TILE, width)
    dma = pltpu.SemaphoreType.DMA
    bf16 = jnp.bfloat16
    line = frames // PAIR
    common = [
        pltpu.VMEM((peers, width, features), bf16),
        pltpu.VMEM((heads, peers, tokens, DH), bf16),
        pltpu.VMEM((tokens, features), F32),
    ]
    common_sems = [
        dma((peers,)), dma((peers,)), dma((heads, peers)), dma((heads, peers)), dma,
    ]
    recv = [pltpu.VMEM((frames * capacity, 2, TILE, DH), bf16)] * heads
    picked = pltpu.VMEM((heads, line, capacity, 2, TILE, DH), bf16)
    passing = [pltpu.VMEM((2, blocks, TILE, DH), bf16)] * (heads * 2 * (line - 1))
    operands = tokens * (3 * width + features) * 2
    needed = operands + sum(
        math.prod(m.shape) * jnp.dtype(m.dtype).itemsize
        for m in common + recv + [picked] + passing
    )
    relayed = frames % PAIR == 0 and needed < VMEM_BYTES * 15 // 16
    if relayed:
        extra = [picked] + [dma((heads, line, 2))] * 4 + [dma((heads, line))] * 2 + passing
    else:
        extra = [
            pltpu.VMEM((slots, frames, capacity, 2, TILE, DH), bf16),
            dma((heads, frames)),
            dma((heads, frames)),
        ]
    dims = (frames, peers, blocks, select, capacity, heads, slots)
    return pl.pallas_call(
        functools.partial(layer_kernel, dims, relayed),
        out_shape=jax.ShapeDtypeStruct((tokens, features), bf16),
        in_specs=[smem, smem, smem, vmem, vmem, vmem, pl.BlockSpec(memory_space=pl.ANY)],
        out_specs=vmem,
        scratch_shapes=common + common_sems + recv + extra,
        compiler_params=pltpu.CompilerParams(
            collective_id=0, has_side_effects=True, vmem_limit_bytes=VMEM_BYTES
        ),
    )(
        pick, my_slot, counts, queries.reshape(tiles), keys.reshape(tiles), values.reshape(tiles),
        w_out,
    )


def solution(mesh):
    placed = (
        P("frames", "heads"),
        P("frames", "heads"),
        P("frames", "heads"),
        P(),
        P("frames"),
        P("heads", None),
    )
    return jax.shard_map(
        shards, mesh=mesh, in_specs=placed, out_specs=P("frames", "heads"), check_vma=False
    )
```

```python
import functools
import math

import jax
import jax.numpy as jnp
from jax import lax
from jax.experimental import pallas as pl
from jax.experimental.pallas import tpu as pltpu
from jax.sharding import PartitionSpec as P

DH = 128
TILE = 128
MESH = pl.DeviceIdType.MESH
F32 = jnp.float32
PAIR = 2
PARTS = 2
UNROLL = 2
AHEAD = 2
VMEM_BYTES = 67043328
NT_DIMS = (((1,), (1,)), ((), ()))


def head_columns(h):
    return slice(h * DH, (h + 1) * DH)


class direct_exchange:
    def __init__(self, dims, pick_ref, k_ref, v_ref, recv, send, kv_send, kv_recv):
        self.frames, _, _, _, self.capacity, self.heads, self.slots = dims
        self.pick_ref, self.k_ref, self.v_ref, self.recv = pick_ref, k_ref, v_ref, recv
        self.send, self.kv_send, self.kv_recv = send, kv_send, kv_recv
        self.me_f, self.me_p = lax.axis_index("frames"), lax.axis_index("heads")

    def copy(self, h, target, origin):
        return pltpu.make_async_remote_copy(
            src_ref=self.send.at[h % self.slots, target],
            dst_ref=self.recv[h].at[pl.ds(origin * self.capacity, self.capacity)],
            send_sem=self.kv_send.at[h, target],
            recv_sem=self.kv_recv.at[h, origin],
            device_id=(target, self.me_p),
            device_id_type=MESH,
        )

    def others(self, action):
        @pl.loop(1, self.frames)
        def _(step):
            action(lax.rem(self.me_f + step, self.frames))

    def pick(self, target, c):
        return self.pick_ref[(target * self.frames + self.me_f) * self.capacity + c]

    def build(self, h):
        if h >= self.slots:
            self.others(lambda target: self.copy(h - self.slots, target, self.me_f).wait_send())

        def fill(target):
            for c in range(self.capacity):
                index = self.pick(target, c)
                self.send[h % self.slots, target, c, 0] = self.k_ref[index, :, head_columns(h)]
                self.send[h % self.slots, target, c, 1] = self.v_ref[index, :, head_columns(h)]

        self.others(fill)
        for c in range(self.capacity):
            index = self.pick(self.me_f, c)
            self.recv[h][self.me_f * self.capacity + c, 0] = self.k_ref[index, :, head_columns(h)]
            self.recv[h][self.me_f * self.capacity + c, 1] = self.v_ref[index, :, head_columns(h)]

    def start(self, h):
        self.others(lambda target: self.copy(h, target, self.me_f).start())

    def prepare(self):
        self.build(0)

    def begin(self):
        self.start(0)

    def follow(self):
        if self.heads > 1:
            self.build(1)
            self.start(1)

    def receive(self, h, midway):
        if h + 2 < self.heads:
            self.build(h + 2)
        midway()
        self.others(lambda origin: self.copy(h, origin, origin).wait_recv())
        if h + 2 < self.heads:
            self.start(h + 2)

    def drain(self):
        for h in range(max(0, self.heads - self.slots), self.heads):
            self.others(lambda target: self.copy(h, target, self.me_f).wait_send())


class relay_exchange:
    def __init__(
        self, dims, pick_ref, k_ref, v_ref, recv,
        picked, up_send, up_recv, down_send, down_recv, x_send, x_recv, *passing,
    ):
        self.frames, _, self.blocks, _, self.capacity, self.heads, _ = dims
        self.line = self.frames // PAIR
        self.pick_ref, self.k_ref, self.v_ref, self.recv = pick_ref, k_ref, v_ref, recv
        self.picked, self.x_send, self.x_recv = picked, x_send, x_recv
        self.sems = ((up_send, up_recv), (down_send, down_recv))
        self.passing = passing
        self.me_f, self.me_p = lax.axis_index("frames"), lax.axis_index("heads")
        self.z, self.x = self.me_f // PAIR, self.me_f % PAIR
        self.partner = self.z * PAIR + (PAIR - 1 - self.x)

    def held(self, h, way, far):
        return self.passing[(h * 2 + way) * (self.line - 1) + far - 1]

    def at(self, way, steps):
        return self.z + steps if way == 0 else self.z - steps

    def inside(self, position):
        return (position >= 0) & (position < self.line)

    def onward(self, h, way, far, kv):
        source = (self.k_ref, self.v_ref)[kv].at[:, :, head_columns(h)]
        if far > 0:
            source = self.held(h, way, far).at[kv]
        send_sem, recv_sem = self.sems[way]
        return pltpu.make_async_remote_copy(
            src_ref=source,
            dst_ref=self.held(h, way, far + 1).at[kv],
            send_sem=send_sem.at[h, far, kv],
            recv_sem=recv_sem.at[h, far, kv],
            device_id=(self.at(way, 1) * PAIR + self.x, self.me_p),
            device_id_type=MESH,
        )

    def beside(self, h, origin_z, column):
        return pltpu.make_async_remote_copy(
            src_ref=self.picked.at[h, origin_z],
            dst_ref=self.recv[h].at[
                pl.ds((origin_z * PAIR + column) * self.capacity, self.capacity)
            ],
            send_sem=self.x_send.at[h, origin_z],
            recv_sem=self.x_recv.at[h, origin_z],
            device_id=(self.partner, self.me_p),
            device_id_type=MESH,
        )

    def send_on(self, h, way, far):
        @pl.when(self.inside(self.at(way, 1)))
        def _():
            for kv in range(2):
                self.onward(h, way, far, kv).start()

    def hand_out(self, h, origin_z, load):
        origin = origin_z * PAIR + self.x
        for c in range(self.capacity):
            theirs = self.pick_ref[(self.partner * self.frames + origin) * self.capacity + c]
            for kv in range(2):
                self.picked[h, origin_z, c, kv] = load(kv, theirs)
        for c in range(self.capacity):
            ours = self.pick_ref[(self.me_f * self.frames + origin) * self.capacity + c]
            for kv in range(2):
                self.recv[h][origin * self.capacity + c, kv] = load(kv, ours)
        self.beside(h, origin_z, self.x).start()

    def own(self, h):
        def load(kv, index):
            return (self.k_ref, self.v_ref)[kv][index, :, head_columns(h)]

        self.hand_out(h, self.z, load)

    def arrive(self, h, far):
        for way in range(2):
            @pl.when(self.inside(self.at(way, -far)))
            def _():
                for kv in range(2):
                    self.onward(h, way, far - 1, kv).wait_recv()
                if far + 1 < self.line:
                    self.send_on(h, way, far)

        for way in range(2):
            @pl.when(self.inside(self.at(way, -far)))
            def _():
                held = self.held(h, way, far)
                self.hand_out(h, self.at(way, -far), lambda kv, index: held[kv, index])

    def prepare(self):
        pass

    def begin(self):
        for h in range(min(AHEAD, self.heads)):
            for way in range(2):
                self.send_on(h, way, 0)

    def follow(self):
        self.own(0)

    def receive(self, h, midway):
        for far in range(1, self.line):
            if far == self.line - 1:
                midway()
            self.arrive(h, far)
            if far == 1 and h + AHEAD < self.heads:
                for way in range(2):
                    self.send_on(h + AHEAD, way, 0)
        if h + 1 < self.heads:
            self.own(h + 1)

        @pl.loop(0, self.line)
        def _(origin_z):
            self.beside(h, origin_z, PAIR - 1 - self.x).wait_recv()

    def drain(self):
        for h in range(self.heads):
            for way in range(2):
                for far in range(self.line - 1):
                    @pl.when(self.inside(self.at(way, -far)) & self.inside(self.at(way, 1)))
                    def _():
                        for kv in range(2):
                            self.onward(h, way, far, kv).wait_send()

            @pl.loop(0, self.line)
            def _(origin_z):
                self.beside(h, origin_z, self.x).wait_send()


def layer_kernel(
    dims, relayed, pick_ref, slot_ref, count_ref, q_ref, k_ref, v_ref, w_ref, out_ref,
    rows, attn, acc, w_send, w_recv, a_send, a_recv, own_sem, *kv_refs,
):
    frames, peers, blocks, select, capacity, heads, slots = dims
    recv, kv_refs = kv_refs[:heads], kv_refs[heads:]
    me_f, me_p = lax.axis_index("frames"), lax.axis_index("heads")
    depth = heads * DH
    features = rows.shape[2]

    barrier = pltpu.get_barrier_semaphore()

    @pl.loop(1, frames)
    def _(step):
        pl.semaphore_signal(
            barrier, inc=1, device_id=(lax.rem(me_f + step, frames), me_p), device_id_type=MESH
        )

    @pl.loop(1, peers)
    def _(step):
        pl.semaphore_signal(
            barrier, inc=1, device_id=(me_f, lax.rem(me_p + step, peers)), device_id_type=MESH
        )

    def columns_of(peer):
        return pl.ds(pl.multiple_of(peer * features, features), features)

    own_rows = pltpu.make_async_copy(w_ref.at[:, columns_of(me_p)], rows.at[me_p], own_sem)
    own_rows.start()

    exchange = (relay_exchange if relayed else direct_exchange)(
        dims, pick_ref, k_ref, v_ref, recv, *kv_refs
    )

    def w_copy(target, origin):
        return pltpu.make_async_remote_copy(
            src_ref=w_ref.at[:, columns_of(target)],
            dst_ref=rows.at[origin],
            send_sem=w_send.at[target],
            recv_sem=w_recv.at[origin],
            device_id=(me_f, target),
            device_id_type=MESH,
        )

    part_blocks = blocks // PARTS
    part_rows = part_blocks * TILE

    def a_copy(h, part, target, origin):
        held = attn.at[h, origin, pl.ds(part * part_rows, part_rows)]
        return pltpu.make_async_remote_copy(
            src_ref=held,
            dst_ref=held,
            send_sem=a_send.at[h, part, target, origin],
            recv_sem=a_recv.at[h, part, origin],
            device_id=(me_f, target),
            device_id_type=MESH,
        )

    twin = me_p + 1 - 2 * lax.rem(me_p, 2)

    def over_alike(action):
        @pl.loop(1, peers // 2)
        def _(step):
            action(lax.rem(me_p + 2 * step, peers))

    def over_twins(action):
        @pl.loop(0, peers // 2)
        def _(step):
            action(lax.rem(twin + 2 * step, peers))

    def share(h, part):
        over_alike(lambda target: a_copy(h, part, target, me_p).start())
        a_copy(h, part, twin, me_p).start()

    def finish(h):
        if h == 0:
            own_rows.wait()
            over_peers(lambda origin: w_copy(origin, origin).wait_recv())
        for part in range(PARTS):

            def relay(origin):
                a_copy(h, part, origin, origin).wait_recv()
                a_copy(h, part, twin, origin).start()

            over_alike(relay)
        for part in range(PARTS):
            over_twins(lambda origin: a_copy(h, part, origin, origin).wait_recv())
            project(h, part)

    def drain_attn(h, part):
        over_alike(lambda target: a_copy(h, part, target, me_p).wait_send())
        a_copy(h, part, twin, me_p).wait_send()
        over_alike(lambda origin: a_copy(h, part, twin, origin).wait_send())

    def over_peers(action):
        @pl.loop(1, peers)
        def _(step):
            action(lax.rem(me_p + step, peers))

    def attend(h, part):
        @pl.loop(part * part_blocks, (part + 1) * part_blocks, unroll=UNROLL)
        def _(b):
            q = q_ref[b, :, head_columns(h)]
            picks = [slot_ref[b * select + s] for s in range(select)]
            keyset = jnp.concatenate(
                [k_ref[b, :, head_columns(h)]] + [recv[h][i, 0] for i in picks], axis=0
            )
            valueset = jnp.concatenate(
                [v_ref[b, :, head_columns(h)]] + [recv[h][i, 1] for i in picks], axis=0
            )
            scores = lax.dot_general(q, keyset, NT_DIMS, preferred_element_type=F32)
            scores = scores * (1.0 / DH**0.5)
            position = lax.broadcasted_iota(jnp.int32, scores.shape, 1)
            scores = jnp.where(position < (count_ref[b] + 1) * TILE, scores, -jnp.inf)
            top = jnp.max(scores, axis=1, keepdims=True)
            probs = jnp.exp(scores - top)
            denom = jnp.sum(probs, axis=1, keepdims=True)
            mixed = jnp.dot(probs.astype(jnp.bfloat16), valueset, preferred_element_type=F32)
            attn[h, me_p, pl.ds(pl.multiple_of(b * TILE, TILE), TILE), :] = (mixed / denom).astype(
                jnp.bfloat16
            )

    row_tile = 2 * TILE

    def project(h, part):
        @pl.loop(part * part_rows // row_tile, (part + 1) * part_rows // row_tile)
        def _(r):
            span = pl.ds(pl.multiple_of(r * row_tile, row_tile), row_tile)
            left = jnp.concatenate([attn[h, p, span, :] for p in range(peers)], axis=1)
            right = jnp.concatenate([rows[p, head_columns(h), :] for p in range(peers)], axis=0)
            term = jnp.dot(left, right, preferred_element_type=F32)
            if h > 0:
                term = term + acc[span, :]
            if h == heads - 1:
                out_ref[span, :] = term.astype(out_ref.dtype)
            else:
                acc[span, :] = term

    exchange.prepare()
    pl.semaphore_wait(barrier, frames + peers - 2)
    exchange.begin()
    over_peers(lambda target: w_copy(target, me_p).start())
    exchange.follow()
    for h in range(heads):
        exchange.receive(h, (lambda: finish(h - 1)) if h > 0 else (lambda: None))
        for part in range(PARTS):
            attend(h, part)
            share(h, part)
    finish(heads - 1)
    exchange.drain()
    over_peers(lambda target: w_copy(target, me_p).wait_send())
    for h in range(heads):
        for part in range(PARTS):
            drain_attn(h, part)


def shards(queries, keys, values, block_ids, counts, w_out):
    frames = lax.axis_size("frames")
    peers = lax.axis_size("heads")
    here = lax.axis_index("frames")
    tokens, width = queries.shape
    blocks = tokens // TILE
    select = block_ids.shape[1]
    heads = width // DH
    requests = blocks * select
    capacity = max(2, (requests + frames - 1) // frames)
    features = w_out.shape[1] // peers
    slots = min(3, heads)

    ids = block_ids.reshape(frames, requests)
    owner = ids // blocks
    order = jnp.arange(requests, dtype=jnp.int32)
    same = (owner[:, :, None] == owner[:, None, :]) & (order[:, None] < order[None, :])
    slot = owner * capacity + jnp.sum(same.astype(jnp.int32), axis=1)
    hit = slot[:, None, :] == jnp.arange(frames * capacity, dtype=jnp.int32)[:, None]
    pick = jnp.sum(jnp.where(hit, (ids % blocks)[:, None, :], 0), axis=2).reshape(-1)
    my_slot = lax.dynamic_slice_in_dim(slot, here, 1, 0).reshape(requests)

    smem = pl.BlockSpec(memory_space=pltpu.SMEM)
    vmem = pl.BlockSpec(memory_space=pltpu.VMEM)
    tiles = (blocks, TILE, width)
    dma = pltpu.SemaphoreType.DMA
    bf16 = jnp.bfloat16
    line = frames // PAIR
    common = [
        pltpu.VMEM((peers, width, features), bf16),
        pltpu.VMEM((heads, peers, tokens, DH), bf16),
        pltpu.VMEM((tokens, features), F32),
    ]
    common_sems = [
        dma((peers,)), dma((peers,)), dma((heads, PARTS, peers, peers)),
        dma((heads, PARTS, peers)), dma,
    ]
    recv = [pltpu.VMEM((frames * capacity, 2, TILE, DH), bf16)] * heads
    picked = pltpu.VMEM((heads, line, capacity, 2, TILE, DH), bf16)
    passing = [pltpu.VMEM((2, blocks, TILE, DH), bf16)] * (heads * 2 * (line - 1))
    operands = tokens * (3 * width + features) * 2
    needed = operands + sum(
        math.prod(m.shape) * jnp.dtype(m.dtype).itemsize
        for m in common + recv + [picked] + passing
    )
    relayed = frames % PAIR == 0 and needed < VMEM_BYTES * 15 // 16
    if relayed:
        extra = [picked] + [dma((heads, line, 2))] * 4 + [dma((heads, line))] * 2 + passing
    else:
        extra = [
            pltpu.VMEM((slots, frames, capacity, 2, TILE, DH), bf16),
            dma((heads, frames)),
            dma((heads, frames)),
        ]
    dims = (frames, peers, blocks, select, capacity, heads, slots)
    return pl.pallas_call(
        functools.partial(layer_kernel, dims, relayed),
        out_shape=jax.ShapeDtypeStruct((tokens, features), bf16),
        in_specs=[smem, smem, smem, vmem, vmem, vmem, pl.BlockSpec(memory_space=pl.ANY)],
        out_specs=vmem,
        scratch_shapes=common + common_sems + recv + extra,
        compiler_params=pltpu.CompilerParams(
            collective_id=0, has_side_effects=True, vmem_limit_bytes=VMEM_BYTES
        ),
    )(
        pick, my_slot, counts, queries.reshape(tiles), keys.reshape(tiles), values.reshape(tiles),
        w_out,
    )


def solution(mesh):
    placed = (
        P("frames", "heads"),
        P("frames", "heads"),
        P("frames", "heads"),
        P(),
        P("frames"),
        P("heads", None),
    )
    return jax.shard_map(
        shards, mesh=mesh, in_specs=placed, out_specs=P("frames", "heads"), check_vma=False
    )
```
